32 devices in a mesh: step: 2 (over y), seq: 16 (over z, x, core).
Axes of the slice: x: 2, y: 2, z: 4, core: 2. Of those that a mesh axis runs over, the one named last changes fastest.
Arguments:
- token_ids: int32 [1536], P('seq'), may hold values from 0 to 64127
- positions: int32 [1536], P('seq'), may hold values from 0 to 511, as said below
- embed_table: bfloat16 [64128, 4096], P('seq', 'step'), may hold values from -6 to 6
- norm_gain: float32 [4096], replicated, may hold values from 0.25 to 1.75
- query_weight: bfloat16 [4096, 4096], P('seq', 'step'), may hold values from -1 to 1
- key_weight: bfloat16 [4096, 1024], P('seq', 'step'), may hold values from -5 to 5
- value_weight: bfloat16 [4096, 1024], P('seq', 'step'), may hold values from -0.09375 to 0.09375
- path_points: float32 [2], replicated, may hold values from 0 to 1
- probe_direction: bfloat16 [1536, 4096], P('seq', 'step'), may hold values from -6 to 6
Outputs:
- attributions: float32 [1536, 4096], P('seq', 'step')
The draws below stay inside these ranges and needn't reach their ends.
Inputs may be any that keep to these rules, and one draw needn't show every extreme that they name: positions[0] is 0 and each later entry is 0 or one more than the entry before; at least one document has exactly 512 tokens.
All inputs are finite; a program needn't handle non-finite values.
Results may differ from the reference program's by a relative error of at most 0.006.
The reference program's roundings to bfloat16 on the way (of `normed`, `attention_bf` and `score_grad`) count: a program that leaves them out, or rounds other values in their place, can miss the bound.
Values may be sent and summed in bfloat16 or wider, within the bound.
A program may use at most 128 MiB of HBM per device.

```python
import math
import jax
import jax.numpy as jnp
import numpy as np
from jax import lax

D = 4096
HEAD = 128
QHEADS = 32
KVHEADS = 8
SEQ_DEV = 96
WINDOW = 512
VOCAB = 64128
TOKENS = 1536
STEPS = 2


def draw_positions(key, part):
    halfway = WINDOW // 2
    anchors = TOKENS // halfway + 1
    base_key = jax.random.fold_in(key, 31)
    key_jitter, key_chosen, key_offset = jax.random.split(base_key, 3)
    jitter = jax.random.randint(key_jitter, (anchors,), 0, halfway + 1)
    chosen = jax.random.randint(key_chosen, (), 0, anchors - 3)
    offset = jax.random.randint(key_offset, (), 1, halfway)
    offset = jnp.where(offset % SEQ_DEV == 0, offset - 1, offset)
    anchor_ids = jnp.arange(anchors, dtype=jnp.int32)
    following = jnp.maximum(jitter, offset)
    jitter = jnp.where(anchor_ids == chosen, offset, jitter)
    jitter = jnp.where(anchor_ids == chosen + 1, halfway + offset, jitter)
    jitter = jnp.where(anchor_ids == chosen + 2, following, jitter)
    starts = anchor_ids * halfway + jitter
    places = jnp.arange(TOKENS, dtype=jnp.int32)
    marked = jnp.any(places[:, None] == starts[None, :], axis=1) | (places == 0)
    latest = lax.cummax(jnp.where(marked, places, 0), axis=0)
    return (places - latest).astype(jnp.int32)


def projection_pair(key):
    base_key = jax.random.fold_in(key, 57)
    key_query, key_other = jax.random.split(base_key)
    fan_scale = D ** (-0.5)
    query_w = jnp.clip(jax.random.normal(key_query, (D, QHEADS * HEAD), jnp.float32), -6.0, 6.0) * fan_scale
    key_w = jnp.clip(jax.random.normal(key_other, (D, KVHEADS * HEAD), jnp.float32), -6.0, 6.0) * fan_scale
    return (query_w, key_w)


def draw_query_weight(key, part):
    return projection_pair(key)[0].astype(jnp.bfloat16)


def draw_key_weight(key, part):
    return projection_pair(key)[1].astype(jnp.bfloat16)


def place_ends(drawn, rng, smallest, largest):
    spot = [jax.random.randint(jax.random.fold_in(rng, axis), (), 0, length) for axis, length in enumerate(drawn.shape)]
    widest = drawn.shape.index(max(drawn.shape))
    beside = spot[:widest] + [(spot[widest] + 1) % drawn.shape[widest]] + spot[widest + 1:]
    return drawn.at[tuple(spot)].set(smallest).at[tuple(beside)].set(largest)


def shard_levels(own_key, shape, shards, smallest, high):
    level, own = 1.0, jax.random.fold_in(own_key, 6)
    for position, parts in shards:
        draws = jnp.exp(jax.random.uniform(jax.random.fold_in(own, position), (parts,), jnp.float32, smallest / len(shards), high / len(shards)))
        level = level * jnp.repeat(draws, shape[position] // parts).reshape([-1 if axis == position else 1 for axis in range(len(shape))])
    return level


def rank_bounds(amount, lean):
    weights = [(1 << 20) // math.isqrt(grade ** lean) + 1 for grade in range(1, amount + 1)]
    deviation = 1 + sum(weights) // (1 << 30)
    return np.cumsum(np.array([max(1, weight // deviation) for weight in weights]))


def skewed_ids(own_key, extent, amount, slope):
    grid = rank_bounds(amount, slope)
    ticket = jax.random.randint(jax.random.fold_in(own_key, 1), extent, 0, int(grid[amount - 1]))
    rank = jnp.searchsorted(jnp.asarray(grid, jnp.int32), ticket, side="right")
    return jax.random.permutation(jax.random.fold_in(own_key, 2), amount)[rank].astype(jnp.int32)


def centred(own_key, shape, scale, reach, pieces=(), kind=jnp.bfloat16):
    array = jax.random.normal(own_key, shape, jnp.float32) * scale
    if len(pieces) > 0:
        array = shard_levels(own_key, shape, pieces, -0.22, 0.18) * array
    return jnp.clip(array, min=-reach, max=reach).astype(kind)


def setup_inputs(seed: int = 0) -> dict:
    keys = jax.random.split(jax.random.key(seed), 10)
    return {
        "token_ids": place_ends(skewed_ids(keys[0], (TOKENS,), VOCAB, 1), jax.random.fold_in(keys[0], 3), 0, VOCAB - 1).astype(jnp.int32),
        "positions": draw_positions(jax.random.fold_in(keys[9], 71), 0),
        "embed_table": centred(keys[2], (VOCAB, D), 1.0, 6.0, ((0, 16), (1, 2))),
        "norm_gain": jnp.clip(1.0 + 0.15 * jax.random.normal(keys[3], (D,), jnp.float32), 0.25, 1.75),
        "query_weight": draw_query_weight(jax.random.fold_in(keys[9], 71), 0),
        "key_weight": draw_key_weight(jax.random.fold_in(keys[9], 71), 0),
        "value_weight": centred(keys[6], (D, KVHEADS * HEAD), D ** -0.5, 0.09375, ((0, 16), (1, 2))),
        "path_points": jnp.clip(jax.random.uniform(keys[7], (STEPS,), jnp.float32, 0.0, 1.0), 0.0, 1.0),
        "probe_direction": centred(keys[8], (TOKENS, QHEADS * HEAD), 1.0, 6.0, ((0, 16), (1, 2))),
    }


NORM_EPSILON = 1e-05
ROPE_BASE = 500000.0
MASKED = -1e+30

def rope_tables(positions, head_size):
    halfway = head_size // 2
    frequency = ROPE_BASE ** (-2.0 * jnp.arange(halfway, dtype=jnp.float32) / head_size)
    angles = positions.astype(jnp.float32)[:, None] * frequency[None, :]
    return (jnp.cos(angles), jnp.sin(angles))

def rotate(vectors, cosine, sinusoid):
    halfway = vectors.shape[-1] // 2
    former = vectors[..., :halfway]
    latter = vectors[..., halfway:]
    cos_rows = cosine[:, None, :]
    sin_rows = sinusoid[:, None, :]
    return jnp.concatenate([former * cos_rows - latter * sin_rows, latter * cos_rows + former * sin_rows], axis=-1)

def unrotate(gradient, cosine, sinusoid):
    halfway = gradient.shape[-1] // 2
    former = gradient[..., :halfway]
    latter = gradient[..., halfway:]
    cos_rows = cosine[:, None, :]
    sin_rows = sinusoid[:, None, :]
    return jnp.concatenate([former * cos_rows + latter * sin_rows, latter * cos_rows - former * sin_rows], axis=-1)

def attend_back(queries, key_rows, value_rows, probe_heads, positions, group_size):
    token_count, head_count, head_size = queries.shape
    shared = key_rows.shape[1]
    block_rows = math.gcd(token_count, 512)
    block_count = token_count // block_rows
    key_span = WINDOW + block_rows
    score_scale = 1.0 / math.sqrt(head_size)
    padding = jnp.zeros((WINDOW, shared, head_size), jnp.float32)
    keys_padded = jnp.concatenate([padding, key_rows.astype(jnp.float32)], axis=0)
    values_padded = jnp.concatenate([padding, value_rows.astype(jnp.float32)], axis=0)
    query_blocks = queries.astype(jnp.float32).reshape(block_count, block_rows, shared, group_size, head_size)
    probe_blocks = probe_heads.astype(jnp.float32).reshape(block_count, block_rows, shared, group_size, head_size)
    position_blocks = positions.reshape(block_count, block_rows)

    def one_block(running, sliced):
        key_grads, value_grads = running
        query_part, probe_part, position_part, which = sliced
        offset = (which * block_rows).astype(jnp.int32)
        key_part = lax.dynamic_slice_in_dim(keys_padded, offset, key_span, 0)
        value_part = lax.dynamic_slice_in_dim(values_padded, offset, key_span, 0)
        query_pos = offset + jnp.arange(block_rows, dtype=jnp.int32)
        key_pos = offset - WINDOW + jnp.arange(key_span, dtype=jnp.int32)
        visible = (key_pos[None, :] <= query_pos[:, None]) & (key_pos[None, :] >= (query_pos - position_part)[:, None])
        scores = jnp.einsum('qgae,kge->gaqk', query_part, key_part) * score_scale
        scores = jnp.where(visible, scores, MASKED)
        row_max = lax.optimization_barrier(jnp.max(scores, axis=-1, keepdims=True))
        powers = jnp.exp(scores - row_max)
        attention = powers / lax.optimization_barrier(jnp.sum(powers, axis=-1, keepdims=True))
        attention_bf = lax.optimization_barrier(attention.astype(jnp.bfloat16)).astype(jnp.float32)
        attention_grad = jnp.einsum('qgae,kge->gaqk', probe_part, value_part)
        row_dot = lax.optimization_barrier(jnp.sum(attention * attention_grad, axis=-1, keepdims=True))
        score_grad = lax.optimization_barrier((attention * (attention_grad - row_dot) * score_scale).astype(jnp.bfloat16)).astype(jnp.float32)
        query_grad = jnp.einsum('gaqk,kge->qgae', score_grad, key_part)
        key_grad = jnp.einsum('gaqk,qgae->kge', score_grad, query_part)
        value_grad = jnp.einsum('gaqk,qgae->kge', attention_bf, probe_part)
        key_grads = lax.dynamic_update_slice_in_dim(key_grads, lax.dynamic_slice_in_dim(key_grads, offset, key_span, 0) + key_grad, offset, 0)
        value_grads = lax.dynamic_update_slice_in_dim(value_grads, lax.dynamic_slice_in_dim(value_grads, offset, key_span, 0) + value_grad, offset, 0)
        return ((key_grads, value_grads), query_grad)
    empty = jnp.zeros((WINDOW + token_count, shared, head_size), jnp.float32)
    indices = jnp.arange(block_count, dtype=jnp.int32)
    (key_grads, value_grads), query_grads = lax.scan(one_block, (empty, empty), (query_blocks, probe_blocks, position_blocks, indices))
    return (query_grads.reshape(token_count, head_count, head_size), key_grads[WINDOW:], value_grads[WINDOW:])

def reference(token_ids, positions, embed_table, norm_gain, query_weight, key_weight, value_weight, path_points, probe_direction):
    embedded = embed_table[token_ids].astype(jnp.float32)
    baseline = embed_table[0].astype(jnp.float32)
    difference = embedded - baseline
    token_count = token_ids.shape[0]
    head_size = HEAD
    group_size = QHEADS // KVHEADS
    cosine, sinusoid = rope_tables(positions, head_size)
    probe_heads = probe_direction.reshape(token_count, QHEADS, head_size)

    def one_step(running, point):
        inputs = baseline[None, :] + point * difference
        radius = jnp.sqrt(lax.optimization_barrier(jnp.mean(inputs * inputs, axis=-1, keepdims=True)) + NORM_EPSILON)
        unitized = inputs / radius
        normed = (unitized * norm_gain).astype(jnp.bfloat16)
        queries = rotate(jnp.dot(normed, query_weight, preferred_element_type=jnp.float32).reshape(token_count, QHEADS, head_size), cosine, sinusoid).astype(jnp.bfloat16)
        key_rows = rotate(jnp.dot(normed, key_weight, preferred_element_type=jnp.float32).reshape(token_count, KVHEADS, head_size), cosine, sinusoid).astype(jnp.bfloat16)
        value_rows = jnp.dot(normed, value_weight, preferred_element_type=jnp.float32).astype(jnp.bfloat16).reshape(token_count, KVHEADS, head_size)
        query_grad, key_grad, value_grad = attend_back(queries, key_rows, value_rows, probe_heads, positions, group_size)
        query_back = unrotate(query_grad, cosine, sinusoid).astype(jnp.bfloat16).reshape(token_count, QHEADS * head_size)
        key_back = unrotate(key_grad, cosine, sinusoid).astype(jnp.bfloat16).reshape(token_count, KVHEADS * head_size)
        value_back = value_grad.astype(jnp.bfloat16).reshape(token_count, KVHEADS * head_size)
        norm_grad = jnp.dot(query_back, query_weight.T, preferred_element_type=jnp.float32)
        norm_grad = norm_grad + jnp.dot(key_back, key_weight.T, preferred_element_type=jnp.float32)
        norm_grad = norm_grad + jnp.dot(value_back, value_weight.T, preferred_element_type=jnp.float32)
        scaled = norm_gain * norm_grad
        input_grad = (scaled - unitized * lax.optimization_barrier(jnp.mean(scaled * unitized, axis=-1, keepdims=True))) / radius
        return (running + input_grad, None)
    summed, _ = lax.scan(one_step, jnp.zeros((token_count, D), jnp.float32), path_points)
    return difference * summed / STEPS
```

```python
import functools
import math

import jax
import jax.numpy as jnp
from jax import lax
from jax.experimental import pallas as pl
from jax.sharding import PartitionSpec as P

HEAD = 128
REACH = 6


NORM_EPSILON = 1e-05
ROPE_BASE = 500000.0
MASKED = -1e30


def passed_along(array, axis, by):
    size = lax.axis_size(axis)
    pairs = [(i, i + by) for i in range(size) if 0 <= i + by < size]
    return lax.ppermute(array, axis, pairs)


def rope_tables(positions, head_size):
    halfway = head_size // 2
    frequency = ROPE_BASE ** (-2.0 * jnp.arange(halfway, dtype=jnp.float32) / head_size)
    angles = positions.astype(jnp.float32)[:, None] * frequency[None, :]
    return (jnp.cos(angles), jnp.sin(angles))


def rotate(vectors, cosine, sinusoid):
    halfway = vectors.shape[-1] // 2
    former = vectors[..., :halfway]
    latter = vectors[..., halfway:]
    cos_rows = cosine[:, None, :]
    sin_rows = sinusoid[:, None, :]
    return jnp.concatenate(
        [former * cos_rows - latter * sin_rows, latter * cos_rows + former * sin_rows], axis=-1
    )


def unrotate(gradient, cosine, sinusoid):
    halfway = gradient.shape[-1] // 2
    former = gradient[..., :halfway]
    latter = gradient[..., halfway:]
    cos_rows = cosine[:, None, :]
    sin_rows = sinusoid[:, None, :]
    return jnp.concatenate(
        [former * cos_rows + latter * sin_rows, latter * cos_rows - former * sin_rows], axis=-1
    )


def token_split(
    token_ids,
    positions,
    embed_table,
    norm_gain,
    query_weight,
    key_weight,
    value_weight,
    path_points,
    probe_direction,
):
    seq_len = token_ids.shape[0]
    step_count = path_points.shape[0]
    head_size = HEAD
    query_heads = query_weight.shape[1] // head_size
    shared_heads = key_weight.shape[1] // head_size
    group_size = query_heads // shared_heads
    query_cols = query_heads * head_size
    shared_cols = shared_heads * head_size
    score_scale = 1.0 / math.sqrt(head_size)
    seq_index = lax.axis_index("seq")
    seq_count = lax.axis_size("seq")
    all_rows = step_count * seq_len
    ids_all = lax.all_gather(token_ids, "seq", axis=0, tiled=True)
    wanted = jnp.concatenate(
        [ids_all.reshape(seq_count, seq_len), jnp.zeros((seq_count, 1), jnp.int32)], axis=1
    ).reshape(seq_count * (seq_len + 1))
    shard_rows = embed_table.shape[0]
    first_row = seq_index * shard_rows
    local = wanted - first_row
    owned = (local >= 0) & (local < shard_rows)
    picked = jnp.take(embed_table, jnp.clip(local, 0, shard_rows - 1), axis=0)
    own_columns = lax.psum_scatter(
        jnp.where(owned[:, None], picked.astype(jnp.float32), 0.0),
        "seq",
        scatter_dimension=0,
        tiled=True,
    )
    looked = lax.all_gather(own_columns.astype(jnp.bfloat16), "step", axis=1, tiled=True).astype(
        jnp.float32
    )
    features = looked.shape[1]
    embedded = looked[:seq_len]
    baseline = looked[seq_len:]
    difference = embedded - baseline
    inputs = baseline[None] + path_points[:, None, None] * difference[None]
    radius = jnp.sqrt(jnp.mean(inputs * inputs, axis=-1, keepdims=True) + NORM_EPSILON)
    unitized = inputs / radius
    normed = (unitized * norm_gain).astype(jnp.bfloat16).reshape(all_rows, features)
    joined = jnp.concatenate([query_weight, key_weight, value_weight], axis=1)
    joined_cols = joined.shape[1]
    projected = jnp.dot(
        normed,
        lax.all_gather(joined, "seq", axis=0, tiled=True),
        preferred_element_type=jnp.float32,
    )
    projected = projected.reshape(step_count, seq_len, joined_cols)
    cosine, sinusoid = rope_tables(positions, head_size)
    queries = rotate(
        projected[..., :query_cols].reshape(step_count, seq_len, query_heads, head_size),
        cosine,
        sinusoid,
    ).astype(jnp.bfloat16)
    key_rows = rotate(
        projected[..., query_cols : query_cols + shared_cols].reshape(
            step_count, seq_len, shared_heads, head_size
        ),
        cosine,
        sinusoid,
    ).astype(jnp.bfloat16)
    key_rows = key_rows.reshape(step_count, seq_len, shared_cols)
    value_rows = projected[..., query_cols + shared_cols :].astype(jnp.bfloat16)
    blocks = [(key_rows, value_rows)]
    current = (key_rows, value_rows)
    for distance in range(REACH):
        current = passed_along((current[0], current[1]), "seq", 1)
        blocks.append(current)
    ordered = blocks[::-1]
    key_all = jnp.concatenate([member[0] for member in ordered], axis=1)
    value_all = jnp.concatenate([member[1] for member in ordered], axis=1)
    reach_keys = key_all.shape[1]
    key_all = key_all.reshape(step_count, reach_keys, shared_heads, head_size)
    value_all = value_all.reshape(step_count, reach_keys, shared_heads, head_size)
    query_pos = seq_index * seq_len + jnp.arange(seq_len, dtype=jnp.int32)
    key_pos = (seq_index - REACH) * seq_len + jnp.arange(reach_keys, dtype=jnp.int32)
    visible = (key_pos[None, :] <= query_pos[:, None]) & (
        key_pos[None, :] >= (query_pos - positions)[:, None]
    )
    query_split = queries.reshape(step_count, seq_len, shared_heads, group_size, head_size)
    probe_split = probe_direction.reshape(seq_len, shared_heads, group_size, head_size)
    scores = (
        jnp.einsum("sqgae,skge->sgaqk", query_split, key_all, preferred_element_type=jnp.float32)
        * score_scale
    )
    scores = jnp.where(visible, scores, MASKED)
    row_max = jnp.max(scores, axis=-1, keepdims=True)
    powers = jnp.exp(scores - row_max)
    attention = powers / jnp.sum(powers, axis=-1, keepdims=True)
    attention_bf = attention.astype(jnp.bfloat16)
    attention_grad = jnp.einsum(
        "qgae,skge->sgaqk", probe_split, value_all, preferred_element_type=jnp.float32
    )
    row_dot = jnp.sum(attention * attention_grad, axis=-1, keepdims=True)
    score_grad = (attention * (attention_grad - row_dot) * score_scale).astype(jnp.bfloat16)
    query_grad = jnp.einsum(
        "sgaqk,skge->sqgae", score_grad, key_all, preferred_element_type=jnp.float32
    )
    query_grad = query_grad.reshape(step_count, seq_len, query_heads, head_size)
    key_grad = jnp.einsum(
        "sgaqk,sqgae->skge", score_grad, query_split, preferred_element_type=jnp.float32
    ).reshape(step_count, reach_keys, shared_cols)
    value_grad = jnp.einsum(
        "sgaqk,qgae->skge", attention_bf, probe_split, preferred_element_type=jnp.float32
    ).reshape(step_count, reach_keys, shared_cols)
    pieces = [
        (
            key_grad[:, which * seq_len : (which + 1) * seq_len],
            value_grad[:, which * seq_len : (which + 1) * seq_len],
        )
        for which in range(REACH + 1)
    ]
    carried = pieces[0]
    for which in range(1, REACH + 1):
        arrived = passed_along(carried, "seq", -1)
        carried = (arrived[0] + pieces[which][0], arrived[1] + pieces[which][1])
    key_total, value_total = carried
    query_back = (
        unrotate(query_grad, cosine, sinusoid).astype(jnp.bfloat16).reshape(all_rows, query_cols)
    )
    key_back = (
        unrotate(key_total.reshape(step_count, seq_len, shared_heads, head_size), cosine, sinusoid)
        .astype(jnp.bfloat16)
        .reshape(all_rows, shared_cols)
    )
    value_back = value_total.astype(jnp.bfloat16).reshape(all_rows, shared_cols)
    joined_grad = jnp.concatenate([query_back, key_back, value_back], axis=1)
    contract = (((1,), (1,)), ((), ()))
    norm_grad = lax.dot_general(
        joined_grad,
        lax.all_gather(joined, "seq", axis=0, tiled=True),
        contract,
        preferred_element_type=jnp.float32,
    )
    scaled = norm_gain * norm_grad.reshape(step_count, seq_len, features)
    input_grad = (scaled - unitized * jnp.mean(scaled * unitized, axis=-1, keepdims=True)) / radius
    partial_value = difference * jnp.sum(input_grad, axis=0) / step_count
    return lax.psum_scatter(partial_value, "step", scatter_dimension=1, tiled=True)


def attend_kernel(scale, reach, q_ref, p_ref, k_ref, v_ref, low_ref, dq_ref, dk_ref, dv_ref):
    rows = q_ref.shape[2]
    span = k_ref.shape[2]
    heads = q_ref.shape[3] // HEAD
    keys = k_ref[0, 0]
    values = v_ref[0, 0]
    across = (((1,), (1,)), ((), ()))
    down = (((0,), (0,)), ((), ()))
    back = lax.broadcasted_iota(jnp.int32, (rows, span), 1) - reach - lax.broadcasted_iota(
        jnp.int32, (rows, span), 0
    )
    visible = (back <= 0) & (back >= -low_ref[0])
    key_sum = jnp.zeros((span, HEAD), jnp.float32)
    value_sum = jnp.zeros((span, HEAD), jnp.float32)
    for head in range(heads):
        cols = slice(head * HEAD, (head + 1) * HEAD)
        query = q_ref[0, 0, :, cols]
        probe = p_ref[0, :, cols]
        scores = lax.dot_general(query, keys, across, preferred_element_type=jnp.float32) * scale
        scores = jnp.where(visible, scores, MASKED)
        powers = jnp.exp(scores - jnp.max(scores, axis=-1, keepdims=True))
        attention = powers / jnp.sum(powers, axis=-1, keepdims=True)
        grads = lax.dot_general(probe, values, across, preferred_element_type=jnp.float32)
        row_dot = jnp.sum(attention * grads, axis=-1, keepdims=True)
        score_grad = (attention * (grads - row_dot) * scale).astype(jnp.bfloat16)
        dq_ref[0, 0, :, cols] = jnp.dot(score_grad, keys, preferred_element_type=jnp.float32)
        key_sum += lax.dot_general(score_grad, query, down, preferred_element_type=jnp.float32)
        value_sum += lax.dot_general(
            attention.astype(jnp.bfloat16), probe, down, preferred_element_type=jnp.float32
        )
    dk_ref[0, 0] = key_sum
    dv_ref[0, 0] = value_sum


def attend_back(queries, probes, key_win, value_win, positions, reach):
    steps, blocks, rows, cols = queries.shape
    span = key_win.shape[2]
    low = positions[:, :, None]
    whole = lambda *tail: pl.BlockSpec((1, 1) + tail, lambda j, s: (s, j, 0, 0))
    shapes = [(rows, cols), (span, HEAD), (span, HEAD)]
    return pl.pallas_call(
        functools.partial(attend_kernel, 1.0 / math.sqrt(HEAD), reach),
        grid=(blocks, steps),
        in_specs=[
            whole(rows, cols),
            pl.BlockSpec((1, rows, cols), lambda j, s: (j, 0, 0)),
            whole(span, HEAD),
            whole(span, HEAD),
            pl.BlockSpec((1, rows, 1), lambda j, s: (j, 0, 0)),
        ],
        out_specs=[whole(*shape) for shape in shapes],
        out_shape=[
            jax.ShapeDtypeStruct((steps, blocks) + shape, jnp.float32) for shape in shapes
        ],
        cost_estimate=pl.CostEstimate(
            flops=10 * steps * blocks * rows * cols * span,
            bytes_accessed=4 * steps * blocks * (rows * cols * 2 + span * HEAD * 4),
            transcendentals=steps * blocks * rows * (cols // HEAD) * span,
        ),
    )(queries, probes, key_win, value_win, low)


def joined_halves(own, other, index):
    first = index == 0
    return jnp.concatenate(
        [jnp.where(first, own, other), jnp.where(first, other, own)], axis=-1
    )


def head_split(
    token_ids,
    positions,
    embed_table,
    norm_gain,
    query_weight,
    key_weight,
    value_weight,
    path_points,
    probe_direction,
):
    seq_len = token_ids.shape[0]
    steps = path_points.shape[0]
    outer = key_weight.shape[1] // HEAD
    group = query_weight.shape[1] // key_weight.shape[1]
    group_cols = group * HEAD
    seq_index = lax.axis_index("seq")
    seq_count = lax.axis_size("seq")
    step_index = lax.axis_index("step")
    inner = seq_count // outer
    mine = seq_index % inner
    far = seq_index // inner
    far_groups = [[o * inner + i for o in range(outer)] for i in range(inner)]
    near_groups = [[o * inner + i for i in range(inner)] for o in range(outer)]
    swap = [(0, 1), (1, 0)]

    both = lax.all_gather(jnp.stack([token_ids, positions]), "seq", axis=0)
    ids_all = both[:, 0]
    block_positions = lax.dynamic_index_in_dim(
        both[:, 1].reshape(outer, inner, seq_len), mine, 1, keepdims=False
    )

    split = lambda array: array.reshape(array.shape[0], outer, -1)
    joined = jnp.concatenate([split(query_weight), split(key_weight), split(value_weight)], axis=2)
    joined = joined.transpose(1, 0, 2)
    traded = [lax.dynamic_index_in_dim(joined, far, 0, keepdims=False)]
    for by in range(1, outer):
        block = lax.dynamic_index_in_dim(joined, (far + by) % outer, 0, keepdims=False)
        ring = [(d, (d + by * inner) % seq_count) for d in range(seq_count)]
        traded.append(lax.ppermute(block, "seq", ring))
    traded = jnp.stack(traded)
    crossed = lax.ppermute(traded, "seq", [(d, d ^ 2) for d in range(seq_count)])
    side = [(d, d ^ 1) for d in range(seq_count)]
    flipped = [
        traded,
        lax.ppermute(traded, "seq", side),
        crossed,
        lax.ppermute(crossed, "seq", side),
    ]
    flipped = jnp.stack(flipped)
    weights = jnp.concatenate(
        [
            lax.dynamic_slice(
                flipped, (mine ^ i, (far - o) % outer, 0, 0), (1, 1) + flipped.shape[2:]
            ).reshape(flipped.shape[2:])
            for o in range(outer)
            for i in range(inner)
        ],
        axis=0,
    )
    probes = lax.all_to_all(
        split(probe_direction).transpose(1, 0, 2), "seq", 0, 0, axis_index_groups=far_groups
    )

    wanted = jnp.pad(ids_all, ((0, 0), (0, 16))).reshape(-1)
    shard_rows = embed_table.shape[0]
    local = wanted - seq_index * shard_rows
    owned = (local >= 0) & (local < shard_rows)
    picked = jnp.take(embed_table, jnp.clip(local, 0, shard_rows - 1), axis=0)
    own_columns = lax.psum_scatter(
        jnp.where(owned[:, None], picked, jnp.zeros((), jnp.bfloat16)),
        "seq",
        scatter_dimension=0,
        tiled=True,
    )
    middle = seq_len // 2
    late = own_columns[:middle]
    late = joined_halves(late, lax.ppermute(late, "step", swap), step_index)
    early = lax.all_gather(own_columns[middle:], "seq", axis=0, axis_index_groups=far_groups)
    late = lax.all_gather(late, "seq", axis=0, axis_index_groups=far_groups)
    early = joined_halves(early, lax.ppermute(early, "step", swap), step_index)
    looked = jnp.concatenate([late, early[:, : seq_len - middle]], axis=1)
    features = looked.shape[2]
    embedded = looked.reshape(outer * seq_len, features).astype(jnp.float32)
    baseline = early[0, seq_len - middle : seq_len - middle + 1].astype(jnp.float32)
    rows = outer * seq_len

    difference = embedded - baseline
    inputs = baseline[None] + path_points[:, None, None] * difference[None]
    radius = jnp.sqrt(jnp.mean(inputs * inputs, axis=-1, keepdims=True) + NORM_EPSILON)
    unitized = inputs / radius
    normed = (unitized * norm_gain).astype(jnp.bfloat16).reshape(steps * rows, features)
    projected = jnp.dot(normed, weights, preferred_element_type=jnp.float32)
    projected = projected.reshape(steps, rows, -1)
    cosine, sinusoid = rope_tables(block_positions.reshape(rows), HEAD)
    queries = rotate(
        projected[..., :group_cols].reshape(steps, rows, group, HEAD), cosine, sinusoid
    ).astype(jnp.bfloat16)
    key_rows = rotate(
        projected[..., group_cols : group_cols + HEAD].reshape(steps, rows, 1, HEAD),
        cosine,
        sinusoid,
    ).astype(jnp.bfloat16)
    value_rows = projected[..., group_cols + HEAD :].astype(jnp.bfloat16)
    shared = jnp.concatenate([key_rows.reshape(steps, rows, HEAD), value_rows], axis=2)
    shared = lax.all_gather(
        shared.reshape(steps, outer, seq_len, 2 * HEAD),
        "seq",
        axis=0,
        axis_index_groups=near_groups,
    )
    shared = shared.transpose(1, 2, 0, 3, 4).reshape(steps, seq_count * seq_len, 2 * HEAD)
    shared = jnp.pad(shared, ((0, 0), (REACH * seq_len, 0), (0, 0)))
    span = (REACH + 1) * seq_len
    starts = [(o * inner + mine) * seq_len for o in range(outer)]
    windows = jnp.stack(
        [lax.dynamic_slice_in_dim(shared, start, span, 1) for start in starts], axis=1
    )
    query_grad, key_grad, value_grad = attend_back(
        queries.reshape(steps, outer, seq_len, group_cols),
        probes,
        windows[..., :HEAD],
        windows[..., HEAD:],
        block_positions,
        REACH * seq_len,
    )
    pairs = jnp.concatenate([key_grad, value_grad], axis=3)
    long = outer * inner * seq_len
    shifted = jnp.zeros((steps, long + REACH * seq_len, 2 * HEAD), jnp.float32)
    for o in range(outer):
        held = lax.dynamic_slice_in_dim(shifted, starts[o], span, 1) + pairs[:, o]
        shifted = lax.dynamic_update_slice_in_dim(shifted, held, starts[o], 1)
    spread = shifted[:, REACH * seq_len :].reshape(steps, outer, inner, seq_len, 2 * HEAD)
    spread = spread.transpose(2, 0, 1, 3, 4).reshape(2, 2, steps * rows, 2 * HEAD)
    kept = lax.dynamic_index_in_dim(spread, mine % 2, 1, keepdims=False)
    sent = lax.dynamic_index_in_dim(spread, 1 - mine % 2, 1, keepdims=False)
    kept = kept + lax.ppermute(sent, "seq", side)
    sent = lax.dynamic_index_in_dim(kept, 1 - mine // 2, 0, keepdims=False)
    kept = lax.dynamic_index_in_dim(kept, mine // 2, 0, keepdims=False)
    total = kept + lax.ppermute(sent, "seq", [(d, d ^ 2) for d in range(seq_count)])
    total = total.reshape(steps, rows, 2 * HEAD)
    query_back = unrotate(query_grad.reshape(steps, rows, group, HEAD), cosine, sinusoid)
    key_back = unrotate(total[..., :HEAD].reshape(steps, rows, 1, HEAD), cosine, sinusoid)
    joined_grad = jnp.concatenate(
        [
            query_back.reshape(steps, rows, group_cols).astype(jnp.bfloat16),
            key_back.reshape(steps, rows, HEAD).astype(jnp.bfloat16),
            total[..., HEAD:].astype(jnp.bfloat16),
        ],
        axis=2,
    ).reshape(steps * rows, -1)
    contract = (((1,), (1,)), ((), ()))
    norm_grad = lax.dot_general(
        joined_grad, weights, contract, preferred_element_type=jnp.float32
    ).reshape(steps, rows, features)
    scaled = norm_gain * norm_grad
    input_grad = (scaled - unitized * jnp.mean(scaled * unitized, axis=-1, keepdims=True)) / radius
    partial_value = difference * jnp.sum(input_grad, axis=0) / steps
    part = features // 2
    stacked = partial_value.reshape(outer, seq_len, features)
    pieces = []
    for begin, end in ((0, middle), (middle, seq_len)):
        piece = stacked[:, begin:end]
        kept = lax.dynamic_slice_in_dim(piece, step_index * part, part, 2)
        given = lax.dynamic_slice_in_dim(piece, (1 - step_index) * part, part, 2)
        arrived = lax.ppermute(given.astype(jnp.bfloat16), "step", swap)
        halved = (kept + arrived.astype(jnp.float32)).astype(jnp.bfloat16)
        pieces.append(
            lax.psum_scatter(
                halved, "seq", scatter_dimension=0, axis_index_groups=far_groups
            ).astype(jnp.float32)
        )
    return jnp.concatenate(pieces, axis=0)


def per_device(*args):
    shared_heads = args[5].shape[1] // HEAD
    fits = shared_heads > 1 and lax.axis_size("seq") == 4 * shared_heads
    if fits and lax.axis_size("step") == 2:
        return head_split(*args)
    return token_split(*args)


def solution(mesh):
    in_specs = (
        P("seq"),
        P("seq"),
        P("seq", "step"),
        P(),
        P("seq", "step"),
        P("seq", "step"),
        P("seq", "step"),
        P(),
        P("seq", "step"),
    )
    out_specs = P("seq", "step")
    return jax.shard_map(
        per_device, mesh=mesh, in_specs=in_specs, out_specs=out_specs, check_vma=False
    )
```
